32 devices in a mesh: dp: 2 (over y), ctx: 8 (over z, x), tp: 2 (over core).
Axes of the slice: x: 2, y: 2, z: 4, core: 2. Of those that a mesh axis runs over, the one named last changes fastest.
Arguments:
- queries: bfloat16 [4, 1024, 4096], P('dp', 'ctx', 'tp'), may hold values from -6 to 6
- keys: bfloat16 [4, 1024, 512], P('dp', 'ctx', 'tp'), may hold values from -6 to 6
- values: bfloat16 [4, 1024, 512], P('dp', 'ctx', 'tp'), may hold values from -6 to 6
- output_gradient: bfloat16 [4, 1024, 4096], P('dp', 'ctx', 'tp'), may hold values from -6 to 6
- sinks: float32 [64], P('tp'), may hold values from -1 to 3
- doc_starts: int32 [4, 64], P('dp'), may hold values from 0 to 2048, as said below
- valid_counts: int32 [4, 8], P('dp'), may hold values from 64 to 128
Outputs:
- query_grad: bfloat16 [4, 1024, 4096], P('dp', 'ctx', 'tp')
- key_grad: bfloat16 [4, 1024, 512], P('dp', 'ctx', 'tp')
- value_grad: bfloat16 [4, 1024, 512], P('dp', 'ctx', 'tp')
- sink_grad: float32 [64], P('tp')
The draws below stay inside these ranges and needn't reach their ends.
Inputs may be any that keep to these rules, and one draw needn't show every extreme that they name: `doc_starts`: each row is strictly increasing, begins with 0 and ends with 2048; a start at or past 1024 opens no document.
All inputs are finite; a program needn't handle non-finite values.
Results may differ from the reference program's by a relative error of at most 0.0093.
Values may be sent and summed in bfloat16 or wider, within the bound.
A program may use at most 64 MiB of HBM per device.

```python
import jax
import jax.numpy as jnp
from jax import lax

QUERY_HEADS = 64
KEY_VALUE_HEADS = 8
HEAD_DIMENSION = 64
WINDOW_LENGTH = 128
CTX_TOK = 128
DOCS = 64
SEQUENCE_LENGTH = 1024
BATCH_SEQUENCES = 4
N_CTX = 8


def draw_queries(key, part):
    regular_portion = jax.random.normal(jax.random.fold_in(key, 1), (BATCH_SEQUENCES, SEQUENCE_LENGTH, QUERY_HEADS * HEAD_DIMENSION), jnp.float32)
    result = jnp.clip(regular_portion, -6.0, 6.0)
    return result.astype(jnp.bfloat16)


def draw_keys(key, part):
    regular_portion = jax.random.normal(jax.random.fold_in(key, 2), (BATCH_SEQUENCES, SEQUENCE_LENGTH, KEY_VALUE_HEADS * HEAD_DIMENSION), jnp.float32)
    result = jnp.clip(regular_portion, -6.0, 6.0)
    return result.astype(jnp.bfloat16)


def draw_doc_starts(key, part):
    spacing = jax.random.randint(jax.random.fold_in(key, 3), (BATCH_SEQUENCES, DOCS), 1, 2 * SEQUENCE_LENGTH // DOCS)
    running = jnp.cumsum(spacing, axis=1)
    starts = (running - spacing[:, :1]).astype(jnp.int32)
    last_column = jnp.arange(DOCS, dtype=jnp.int32)[None, :] == DOCS - 1
    return jnp.where(last_column, jnp.int32(2 * SEQUENCE_LENGTH), starts).astype(jnp.int32)


def place_ends(values, stream_key, least, top_value):
    longest = values.shape.index(max(values.shape))
    spots = []
    for shift in (0, 1):
        where = [jax.random.randint(jax.random.fold_in(stream_key, axis), (), 0, length) for axis, length in enumerate(values.shape)]
        where[longest] = (where[longest] + shift) % values.shape[longest]
        spots.append(tuple(where))
    return values.at[spots[0]].set(least).at[spots[1]].set(top_value)


def level_of(own_key, extent, cuts, low, top_value):
    loudness, own = 1.0, jax.random.fold_in(own_key, 6)
    for dim, shards_of in cuts:
        heights = jnp.exp(jax.random.uniform(jax.random.fold_in(own, dim), (shards_of,), jnp.float32, low / len(cuts), top_value / len(cuts)))
        loudness = loudness * jnp.repeat(heights, extent[dim] // shards_of).reshape([-1 if axis == dim else 1 for axis in range(len(extent))])
    return loudness


def normal_values(rng, dims, width, reach, shards=(), held_as=jnp.bfloat16):
    drawn = jax.random.normal(rng, dims, jnp.float32) * width
    if len(shards) > 0:
        drawn = level_of(rng, dims, shards, -0.22, 0.18) * drawn
    return jnp.clip(drawn, min=-reach, max=reach).astype(held_as)


def setup_inputs(seed: int = 0) -> dict:
    seeds = jax.random.split(jax.random.key(seed), 8)
    queries = draw_queries(jax.random.fold_in(seeds[7], 71), 0)
    keys = draw_keys(jax.random.fold_in(seeds[7], 71), 0)
    values = normal_values(seeds[2], (BATCH_SEQUENCES, SEQUENCE_LENGTH, KEY_VALUE_HEADS * HEAD_DIMENSION), 1.0, 6.0, ((0, 2), (1, 8), (2, 2)))
    output_gradient = normal_values(seeds[3], (BATCH_SEQUENCES, SEQUENCE_LENGTH, QUERY_HEADS * HEAD_DIMENSION), 1.0, 6.0, ((0, 2), (1, 8), (2, 2)))
    sinks = jnp.clip(-1.0 + 4.0 * jax.random.uniform(seeds[4], (QUERY_HEADS,), jnp.float32) ** level_of(seeds[4], (QUERY_HEADS,), ((0, 2),), -0.2, 0.2), -1.0, 3.0)
    doc_starts = draw_doc_starts(jax.random.fold_in(seeds[7], 71), 0)
    valid_counts = place_ends(jax.random.randint(seeds[6], (BATCH_SEQUENCES, N_CTX), CTX_TOK - WINDOW_LENGTH // 2, CTX_TOK + 1), jax.random.fold_in(seeds[6], 1), CTX_TOK - WINDOW_LENGTH // 2, CTX_TOK).astype(jnp.int32)
    return dict(queries=queries, keys=keys, values=values, output_gradient=output_gradient, sinks=sinks, doc_starts=doc_starts, valid_counts=valid_counts)


masked_score = -1e30


def document_ids(starts, positions):
    return jnp.sum((starts[None, :] <= positions[:, None]).astype(jnp.int32), axis=1)


def key_valid_mask(counts, positions, block_rows):
    block_index = positions // block_rows
    offset = positions - block_index * block_rows
    matches = jnp.arange(counts.shape[0], dtype=jnp.int32)[None, :] == block_index[:, None]
    limits = jnp.sum(jnp.where(matches, counts[None, :], 0), axis=1)
    return offset < limits


def band_grads(query_tile_block, key_tile_block, value_tile_block, output_grad_block, query_pos, key_pos, query_doc, key_doc, key_valid, sink_logits):
    heads_kv = key_tile_block.shape[2]
    query_group_width = query_tile_block.shape[3]
    scaling = query_tile_block.shape[4] ** -0.5
    query_wide = query_tile_block.astype(jnp.float32)
    key_wide = key_tile_block.astype(jnp.float32)
    value_wide = value_tile_block.astype(jnp.float32)
    grad_wide = output_grad_block.astype(jnp.float32)
    scores = jnp.einsum('nqhgd,nkhd->nhgqk', query_wide, key_wide) * scaling
    allowed = (key_pos[:, None, :] <= query_pos[:, :, None]) & (query_pos[:, :, None] - key_pos[:, None, :] < WINDOW_LENGTH)
    allowed = allowed & (query_doc[:, :, None] == key_doc[:, None, :]) & key_valid[:, None, :]
    scores = jnp.where(allowed[:, None, None], scores, masked_score)
    sink_term = sink_logits.reshape(heads_kv, query_group_width)[None, :, :, None]
    maxima = jnp.maximum(jnp.max(scores, axis=-1), sink_term)
    powers = jnp.exp(scores - maxima[..., None])
    sink_exp = jnp.exp(sink_term - maxima)
    denominator = jnp.sum(powers, axis=-1) + sink_exp
    attend = powers / denominator[..., None]
    attend_low = lax.optimization_barrier(attend.astype(jnp.bfloat16)).astype(jnp.float32)
    context = jnp.einsum('nhgqk,nkhd->nhgqd', attend_low, value_wide)
    deltas = jnp.sum(jnp.transpose(grad_wide, (0, 2, 3, 1, 4)) * context, axis=-1)
    grad_attend = jnp.einsum('nqhgd,nkhd->nhgqk', grad_wide, value_wide)
    grad_score = attend * (grad_attend - deltas[..., None])
    score_low = lax.optimization_barrier(grad_score.astype(jnp.bfloat16)).astype(jnp.float32)
    query_grad = jnp.einsum('nhgqk,nkhd->nqhgd', score_low, key_wide) * scaling
    key_grad = jnp.einsum('nhgqk,nqhgd->nkhd', score_low, query_wide) * scaling
    value_grad = jnp.einsum('nhgqk,nqhgd->nkhd', attend_low, grad_wide)
    sink_grad = -jnp.sum(sink_exp / denominator * deltas, axis=-1)
    return query_grad, key_grad, value_grad, sink_grad.reshape(sink_grad.shape[0], heads_kv * query_group_width)


def paired_block_tiles(sequence_rows, block_tiles, heads_kv):
    padded = jnp.concatenate([jnp.zeros((WINDOW_LENGTH, heads_kv * HEAD_DIMENSION), sequence_rows.dtype), sequence_rows], axis=0)
    padded = padded.reshape(block_tiles + 1, WINDOW_LENGTH, heads_kv, HEAD_DIMENSION)
    return jnp.concatenate([padded[:-1], padded[1:]], axis=1)


def reference(queries, keys, values, output_gradient, sinks, doc_starts, valid_counts):
    block_tiles = SEQUENCE_LENGTH // WINDOW_LENGTH
    query_group_width = QUERY_HEADS // KEY_VALUE_HEADS
    query_lines = jnp.arange(SEQUENCE_LENGTH, dtype=jnp.int32).reshape(block_tiles, WINDOW_LENGTH)
    key_lines = jnp.arange(-WINDOW_LENGTH, SEQUENCE_LENGTH, dtype=jnp.int32).reshape(block_tiles + 1, WINDOW_LENGTH)
    key_lines = jnp.concatenate([key_lines[:-1], key_lines[1:]], axis=1)
    query_list = []
    key_block_items = []
    value_block_items = []
    sink_total = jnp.zeros((QUERY_HEADS,), jnp.float32)
    for sequence_index in range(BATCH_SEQUENCES):
        query_doc = document_ids(doc_starts[sequence_index], query_lines.reshape(-1)).reshape(block_tiles, WINDOW_LENGTH)
        key_doc = document_ids(doc_starts[sequence_index], key_lines.reshape(-1)).reshape(block_tiles, 2 * WINDOW_LENGTH)
        key_valid = key_valid_mask(valid_counts[sequence_index], key_lines.reshape(-1), CTX_TOK).reshape(block_tiles, 2 * WINDOW_LENGTH)
        query_tile_block = queries[sequence_index].reshape(block_tiles, WINDOW_LENGTH, KEY_VALUE_HEADS, query_group_width, HEAD_DIMENSION)
        output_grad_block = output_gradient[sequence_index].reshape(block_tiles, WINDOW_LENGTH, KEY_VALUE_HEADS, query_group_width, HEAD_DIMENSION)
        key_tile_block = paired_block_tiles(keys[sequence_index], block_tiles, KEY_VALUE_HEADS)
        value_tile_block = paired_block_tiles(values[sequence_index], block_tiles, KEY_VALUE_HEADS)

        def per_block(entries):
            results = band_grads(*[member[None] for member in entries], sinks)
            return tuple(member[0] for member in results)

        dq_all, dk_all, dv_all, sink_part = lax.map(per_block, (query_tile_block, key_tile_block, value_tile_block, output_grad_block, query_lines, key_lines, query_doc, key_doc, key_valid))
        key_grad_overall = dk_all[:, WINDOW_LENGTH:] + jnp.concatenate([dk_all[1:, :WINDOW_LENGTH], jnp.zeros_like(dk_all[:1, :WINDOW_LENGTH])], axis=0)
        value_grad_overall = dv_all[:, WINDOW_LENGTH:] + jnp.concatenate([dv_all[1:, :WINDOW_LENGTH], jnp.zeros_like(dv_all[:1, :WINDOW_LENGTH])], axis=0)
        query_list.append(dq_all.reshape(SEQUENCE_LENGTH, QUERY_HEADS * HEAD_DIMENSION).astype(jnp.bfloat16))
        key_block_items.append(key_grad_overall.reshape(SEQUENCE_LENGTH, KEY_VALUE_HEADS * HEAD_DIMENSION).astype(jnp.bfloat16))
        value_block_items.append(value_grad_overall.reshape(SEQUENCE_LENGTH, KEY_VALUE_HEADS * HEAD_DIMENSION).astype(jnp.bfloat16))
        sink_total = sink_total + jnp.sum(sink_part, axis=0)
    return (jnp.stack(query_list), jnp.stack(key_block_items), jnp.stack(value_block_items), sink_total)
```

```python
import functools

import jax
import jax.numpy as jnp
from jax import lax
from jax.experimental import pallas as pl
from jax.experimental.pallas import tpu as pltpu
from jax.sharding import PartitionSpec as P

HEAD = 64
WINDOW = 128
LANES = 128
HALF = WINDOW // 2
SPAN = WINDOW + HALF
masked_score = -1e30
MESH = pl.DeviceIdType.MESH
F32 = jnp.float32
BF16 = jnp.bfloat16

NT_DIMS = (((1,), (1,)), ((), ()))


def mm(a, b):
    return jnp.dot(a, b, preferred_element_type=F32)


def mm_nt(a, b):
    return lax.dot_general(a, b, NT_DIMS, preferred_element_type=F32)


def kernel(
    n_dp, n_ctx, seqs, pairs,
    q_ref, k_ref, v_ref, g_ref, sinks_ref, starts_ref, counts_ref,
    dq_ref, dk_ref, dv_ref, sg_ref,
    qbuf, gbuf, kvown, kvhalo, dqbuf, bias, gsend, grecv, gown, sacc, ssend, srecv,
    in_sem, out_sem, hs_sem, hr_sem, gs_sem, gr_sem, ss_sem, sr_sem,
):
    dp, ctx, tp = lax.axis_index("dp"), lax.axis_index("ctx"), lax.axis_index("tp")
    chunks = seqs * pairs
    group = n_dp * n_ctx
    me = dp * n_ctx + ctx
    qw = q_ref.shape[2] // pairs
    docs = starts_ref.shape[1]
    n_sinks = sinks_ref.shape[0]
    scale = HEAD ** -0.5

    def peer(i):
        other = lax.rem(me + i, group)
        return (other // n_ctx, lax.rem(other, n_ctx), tp)

    barrier = pltpu.get_barrier_semaphore()

    def greet(i, carry):
        pl.semaphore_signal(barrier, inc=1, device_id=peer(i), device_id_type=MESH)
        return carry

    lax.fori_loop(1, group, greet, 0)

    def local_copies(t):
        b, cp = t // pairs, lax.rem(t, pairs)
        wide = pl.ds(pl.multiple_of(cp * qw, LANES), qw)
        thin = pl.ds(pl.multiple_of(cp * LANES, LANES), LANES)
        return (
            pltpu.make_async_copy(k_ref.at[b, :, thin], kvown.at[0, t], in_sem.at[0, t]),
            pltpu.make_async_copy(v_ref.at[b, :, thin], kvown.at[1, t], in_sem.at[1, t]),
            pltpu.make_async_copy(q_ref.at[b, :, wide], qbuf.at[t], in_sem.at[2, t]),
            pltpu.make_async_copy(g_ref.at[b, :, wide], gbuf.at[t], in_sem.at[3, t]),
        )

    for t in range(chunks):
        for copy in local_copies(t):
            copy.start()

    def out_copy(t):
        b, cp = t // pairs, lax.rem(t, pairs)
        wide = pl.ds(pl.multiple_of(cp * qw, LANES), qw)
        return pltpu.make_async_copy(dqbuf.at[t], dq_ref.at[b, :, wide], out_sem.at[t])

    def halo_copies(t):
        b, cp = t // pairs, lax.rem(t, pairs)
        thin = pl.ds(pl.multiple_of(cp * LANES, LANES), LANES)
        target = (dp, lax.rem(ctx + 1, n_ctx), tp)
        return tuple(
            pltpu.make_async_remote_copy(
                src_ref=ref.at[b, :, thin], dst_ref=kvhalo.at[w, t],
                send_sem=hs_sem.at[w, t], recv_sem=hr_sem.at[w, t],
                device_id=target, device_id_type=MESH,
            )
            for w, ref in enumerate((k_ref, v_ref))
        )

    def grad_copies(t):
        target = (dp, lax.rem(ctx + n_ctx - 1, n_ctx), tp)
        return tuple(
            pltpu.make_async_remote_copy(
                src_ref=gsend.at[w, t], dst_ref=grecv.at[w, t],
                send_sem=gs_sem.at[w, t], recv_sem=gr_sem.at[w, t],
                device_id=target, device_id_type=MESH,
            )
            for w in range(2)
        )

    def sink_copy(i):
        return pltpu.make_async_remote_copy(
            src_ref=ssend, dst_ref=srecv.at[i - 1],
            send_sem=ss_sem.at[i - 1], recv_sem=sr_sem.at[i - 1],
            device_id=peer(i), device_id_type=MESH,
        )

    lane = lax.broadcasted_iota(jnp.int32, (1, LANES), 1)
    low_lane = lane < HEAD
    start = ctx * WINDOW
    for b in range(seqs):
        fold = lax.rem(lane, HALF)
        pos_parts = [start + fold, start + HALF + fold, start - WINDOW + lane, start + lane]
        ids = [jnp.zeros((1, LANES), F32) for _ in pos_parts]
        for d in range(docs):
            s = starts_ref[b, d]
            ids = [x + (s <= pos).astype(F32) for x, pos in zip(ids, pos_parts)]
        key_doc = jnp.concatenate(
            [jnp.transpose(jnp.broadcast_to(x, (LANES, LANES))) for x in ids[2:]], axis=0
        )
        krow = lax.broadcasted_iota(jnp.int32, (2 * WINDOW, LANES), 0)
        kpos = krow - WINDOW
        prev_limit = counts_ref[b, lax.rem(ctx + n_ctx - 1, n_ctx)]
        own_limit = counts_ref[b, ctx]
        first = (ctx == 0).astype(jnp.int32)
        limit = jnp.where(krow < WINDOW, prev_limit * (1 - first), own_limit + WINDOW)
        valid = krow < limit
        for h in range(2):
            qpos = jnp.broadcast_to(h * HALF + fold, (2 * WINDOW, LANES))
            ok = (kpos <= qpos) & (qpos - kpos < WINDOW) & valid & (key_doc == ids[h])
            whole = jnp.where(ok, 0.0, masked_score).astype(F32)
            bias[b, h] = whole[h * HALF : h * HALF + SPAN]

    sacc[...] = jnp.zeros_like(sacc)

    pl.semaphore_wait(barrier, group - 1)

    @pl.when(ctx < n_ctx - 1)
    def _():
        for t in range(chunks):
            for copy in halo_copies(t):
                copy.start()

    @pl.when(ctx == 0)
    def _():
        kvhalo[...] = jnp.zeros_like(kvhalo)

    keep0 = low_lane.astype(F32).astype(BF16)
    keep1 = (1.0 - low_lane.astype(F32)).astype(BF16)

    def spread(tile, ci):
        wide = tile.astype(F32)
        turned = pltpu.roll(wide, HEAD, 1)
        return jnp.where(low_lane, wide, turned) if ci == 0 else jnp.where(low_lane, turned, wide)

    def step(t, carry):
        b, cp = t // pairs, lax.rem(t, pairs)
        for copy in local_copies(t):
            copy.wait()

        @pl.when(ctx > 0)
        def _():
            for copy in halo_copies(t):
                copy.wait_recv()

        kpair = jnp.concatenate([kvhalo[0, t], kvown[0, t]], axis=0)
        vpair = jnp.concatenate([kvhalo[1, t], kvown[1, t]], axis=0)
        sums = []
        for ci in range(2):
            kwide = spread(kpair, ci) * scale
            k2 = kwide.astype(BF16)
            v2 = spread(vpair, ci).astype(BF16)
            dk_parts, dv_parts = [], []
            for h in range(2):
                r0 = h * HALF
                kcut, vcut = k2[r0 : r0 + SPAN], v2[r0 : r0 + SPAN]
                turned = kwide if h == 0 else jnp.concatenate([kwide[HALF:], kwide[:HALF]], axis=0)
                kt = jnp.transpose(turned)[:HEAD, :SPAN].astype(BF16)
                band = bias[b, h]
                band = jnp.concatenate([band, band], axis=1)
                wq_all, wg_all, p_all, d_all = [], [], [], []
                for quad in range(2):
                    base = ci * (qw // 2) + quad * 2 * LANES
                    qs = [qbuf[t, r0 : r0 + HALF, base + p * LANES : base + (p + 1) * LANES] for p in range(2)]
                    gs = [gbuf[t, r0 : r0 + HALF, base + p * LANES : base + (p + 1) * LANES] for p in range(2)]
                    wq = jnp.concatenate([x * keep for keep in (keep0, keep1) for x in qs], axis=0)
                    wg = jnp.concatenate([x * keep for keep in (keep0, keep1) for x in gs], axis=0)
                    head0 = (cp * 2 + ci) * (n_sinks // (2 * pairs)) + quad * 4
                    sink = jnp.concatenate(
                        [
                            jnp.where(low_lane, sinks_ref[head0 + e], sinks_ref[head0 + 2 + e])
                            for e in range(2)
                        ],
                        axis=1,
                    )
                    scores = mm_nt(kcut, wq) + band
                    top = jnp.maximum(jnp.max(scores, axis=0, keepdims=True), sink)
                    powers = jnp.exp(scores - top)
                    sink_exp = jnp.exp(sink - top)
                    inv = 1.0 / (jnp.sum(powers, axis=0, keepdims=True) + sink_exp)
                    prob = powers * inv
                    dprob = mm_nt(vcut, wg)
                    delta = jnp.sum(prob * dprob, axis=0, keepdims=True)
                    dscore = (prob * (dprob - delta)).astype(BF16)
                    dqt = mm(kt, dscore)
                    dq2 = jnp.transpose(jnp.concatenate([dqt[:, :LANES], dqt[:, LANES:]], axis=0)).astype(BF16)
                    for p in range(2):
                        dqbuf[t, r0 : r0 + HALF, base + p * LANES : base + (p + 1) * LANES] = dq2[
                            p * HALF : (p + 1) * HALF
                        ]
                    row = ci * 2 + quad
                    sacc[cp, row : row + 1, :] -= sink_exp * inv * delta
                    wq_all.append(wq)
                    wg_all.append(wg)
                    p_all.append(prob.astype(BF16))
                    d_all.append(dscore)
                dv_parts.append(mm(jnp.concatenate(p_all, axis=1), jnp.concatenate(wg_all, axis=0)))
                dk_parts.append(mm(jnp.concatenate(d_all, axis=1), jnp.concatenate(wq_all, axis=0)))
            totals = []
            for lo, hi in (dk_parts, dv_parts):
                x = jnp.concatenate([lo[:HALF], lo[HALF:] + hi[:WINDOW], hi[WINDOW:]], axis=0)
                totals.append(x + pltpu.roll(x, HEAD, 1))
            sums.append(totals)
        for w in range(2):
            x = jnp.where(low_lane, sums[0][w], sums[1][w])
            if w == 0:
                x = x * scale
            gsend[w, t] = x[:WINDOW].astype(BF16)
            gown[w, t] = x[WINDOW:]

        @pl.when(ctx > 0)
        def _():
            for copy in grad_copies(t):
                copy.start()

        out_copy(t).start()
        return carry

    lax.fori_loop(0, chunks, step, 0)

    lane4 = lax.broadcasted_iota(jnp.int32, (4, LANES), 1)
    row4 = lax.broadcasted_iota(jnp.int32, (4, LANES), 0)
    mine = jnp.zeros((1, LANES), F32)
    for cp in range(pairs):
        part = sacc[cp]
        for e in range(2):
            cut = part[:, e * LANES : (e + 1) * LANES]
            for p in range(2):
                chosen = low_lane if p == 0 else jnp.logical_not(low_lane)
                seg = jnp.sum(jnp.where(chosen, cut, 0.0), axis=1, keepdims=True)
                spot = lane4 == cp * 16 + row4 * 4 + p * 2 + e
                mine = mine + jnp.sum(jnp.where(spot, seg, 0.0), axis=0, keepdims=True)
    ssend[...] = jnp.broadcast_to(mine, ssend.shape)

    def send_sink(i, carry):
        sink_copy(i).start()
        return carry

    lax.fori_loop(1, group, send_sink, 0)

    for t in range(chunks):
        b, cp = t // pairs, t % pairs
        cut = slice(cp * LANES, (cp + 1) * LANES)

        @pl.when(ctx < n_ctx - 1)
        def _():
            for copy in grad_copies(t):
                copy.wait_recv()
            for w, ref in enumerate((dk_ref, dv_ref)):
                ref[b, :, cut] = (gown[w, t] + grecv[w, t].astype(F32)).astype(BF16)

        @pl.when(ctx == n_ctx - 1)
        def _():
            for w, ref in enumerate((dk_ref, dv_ref)):
                ref[b, :, cut] = gown[w, t].astype(BF16)

    @pl.when(ctx < n_ctx - 1)
    def _():
        for t in range(chunks):
            for copy in halo_copies(t):
                copy.wait_send()

    @pl.when(ctx > 0)
    def _():
        for t in range(chunks):
            for copy in grad_copies(t):
                copy.wait_send()

    for t in range(chunks):
        out_copy(t).wait()

    def take_sink(i, total):
        sink_copy(i).wait()
        return total + srecv[i - 1]

    total = lax.fori_loop(1, group, take_sink, ssend[...])
    sg_ref[...] = total[:1, : sg_ref.shape[1]]


def local(n_dp, n_ctx, queries, keys, values, output_gradient, sinks, doc_starts, valid_counts):
    seqs, rows, query_width = queries.shape
    kv_width = keys.shape[2]
    assert rows == WINDOW and kv_width % LANES == 0
    pairs = kv_width // LANES
    assert query_width == kv_width * 8
    chunks = seqs * pairs
    group = n_dp * n_ctx
    any_spec = pl.BlockSpec(memory_space=pl.ANY)
    smem = pl.BlockSpec(memory_space=pltpu.SMEM)
    vmem = pl.BlockSpec(memory_space=pltpu.VMEM)
    wide = query_width // pairs
    dq, dk, dv, sg = pl.pallas_call(
        functools.partial(kernel, n_dp, n_ctx, seqs, pairs),
        out_shape=(
            jax.ShapeDtypeStruct(queries.shape, BF16),
            jax.ShapeDtypeStruct(keys.shape, BF16),
            jax.ShapeDtypeStruct(values.shape, BF16),
            jax.ShapeDtypeStruct((1, sinks.shape[0]), F32),
        ),
        in_specs=[any_spec] * 4 + [smem] * 3,
        out_specs=(any_spec, vmem, vmem, vmem),
        scratch_shapes=[
            pltpu.VMEM((chunks, rows, wide), BF16),
            pltpu.VMEM((chunks, rows, wide), BF16),
            pltpu.VMEM((2, chunks, rows, LANES), BF16),
            pltpu.VMEM((2, chunks, rows, LANES), BF16),
            pltpu.VMEM((chunks, rows, wide), BF16),
            pltpu.VMEM((seqs, 2, SPAN, LANES), F32),
            pltpu.VMEM((2, chunks, rows, LANES), BF16),
            pltpu.VMEM((2, chunks, rows, LANES), BF16),
            pltpu.VMEM((2, chunks, rows, LANES), F32),
            pltpu.VMEM((pairs, 4, 2 * LANES), F32),
            pltpu.VMEM((8, LANES), F32),
            pltpu.VMEM((group - 1, 8, LANES), F32),
            pltpu.SemaphoreType.DMA((4, chunks)),
            pltpu.SemaphoreType.DMA((chunks,)),
            pltpu.SemaphoreType.DMA((2, chunks)),
            pltpu.SemaphoreType.DMA((2, chunks)),
            pltpu.SemaphoreType.DMA((2, chunks)),
            pltpu.SemaphoreType.DMA((2, chunks)),
            pltpu.SemaphoreType.DMA((group - 1,)),
            pltpu.SemaphoreType.DMA((group - 1,)),
        ],
        compiler_params=pltpu.CompilerParams(
            collective_id=0, has_side_effects=True, vmem_limit_bytes=48 * 1024 * 1024
        ),
    )(queries, keys, values, output_gradient, sinks, doc_starts, valid_counts)
    return dq, dk, dv, sg.reshape(sinks.shape)


def solution(mesh):
    placed = (
        P("dp", "ctx", "tp"),
        P("dp", "ctx", "tp"),
        P("dp", "ctx", "tp"),
        P("dp", "ctx", "tp"),
        P("tp"),
        P("dp", None),
        P("dp", None),
    )
    return jax.shard_map(
        functools.partial(local, mesh.shape["dp"], mesh.shape["ctx"]),
        mesh=mesh,
        in_specs=placed,
        out_specs=(P("dp", "ctx", "tp"), P("dp", "ctx", "tp"), P("dp", "ctx", "tp"), P("tp")),
        check_vma=False,
    )
```

```python
import functools

import jax
import jax.numpy as jnp
from jax import lax
from jax.experimental import pallas as pl
from jax.experimental.pallas import tpu as pltpu
from jax.sharding import PartitionSpec as P

HEAD = 64
WINDOW = 128
LANES = 128
HALF = WINDOW // 2
SPAN = WINDOW + HALF
masked_score = -1e30
MESH = pl.DeviceIdType.MESH
F32 = jnp.float32
BF16 = jnp.bfloat16

NT_DIMS = (((1,), (1,)), ((), ()))


def mm(a, b):
    return jnp.dot(a, b, preferred_element_type=F32)


def mm_nt(a, b):
    return lax.dot_general(a, b, NT_DIMS, preferred_element_type=F32)


def kernel(
    n_dp, n_ctx, seqs, pairs,
    q_ref, k_ref, v_ref, g_ref, sinks_in, starts_in, counts_in,
    dq_ref, dk_ref, dv_ref, sg_ref,
    qbuf, gbuf, kvown, kvhalo, sinks_ref, starts_ref, counts_ref, bias, gsend, grecv, gown, sacc, ssend, srecv,
    in_sem, small_sem, hs_sem, hr_sem, gs_sem, gr_sem, ss_sem, sr_sem,
):
    dp, ctx, tp = lax.axis_index("dp"), lax.axis_index("ctx"), lax.axis_index("tp")
    chunks = seqs * pairs
    group = n_dp * n_ctx
    me = dp * n_ctx + ctx
    qw = q_ref.shape[2] // pairs
    docs = starts_ref.shape[1]
    n_sinks = sinks_ref.shape[0]
    scale = HEAD ** -0.5

    def peer(i):
        other = lax.rem(me + i, group)
        return (other // n_ctx, lax.rem(other, n_ctx), tp)

    barrier = pltpu.get_barrier_semaphore()

    def greet(i, carry):
        pl.semaphore_signal(barrier, inc=1, device_id=peer(i), device_id_type=MESH)
        return carry

    lax.fori_loop(1, group, greet, 0)

    def local_copies(t):
        b, cp = t // pairs, lax.rem(t, pairs)
        wide = pl.ds(pl.multiple_of(cp * qw, LANES), qw)
        thin = pl.ds(pl.multiple_of(cp * LANES, LANES), LANES)
        return (
            pltpu.make_async_copy(k_ref.at[b, :, thin], kvown.at[0, t], in_sem.at[0, t]),
            pltpu.make_async_copy(v_ref.at[b, :, thin], kvown.at[1, t], in_sem.at[1, t]),
            pltpu.make_async_copy(q_ref.at[b, :, wide], qbuf.at[t], in_sem.at[2, t]),
            pltpu.make_async_copy(g_ref.at[b, :, wide], gbuf.at[t], in_sem.at[3, t]),
        )

    smalls = [
        pltpu.make_async_copy(src, dst, small_sem.at[i])
        for i, (src, dst) in enumerate(
            ((sinks_in, sinks_ref), (starts_in, starts_ref), (counts_in, counts_ref))
        )
    ]
    for copy in smalls:
        copy.start()
    for t in range(chunks):
        for copy in local_copies(t):
            copy.start()
    for copy in smalls:
        copy.wait()

    def halo_copies(t):
        b, cp = t // pairs, lax.rem(t, pairs)
        thin = pl.ds(pl.multiple_of(cp * LANES, LANES), LANES)
        target = (dp, lax.rem(ctx + 1, n_ctx), tp)
        return tuple(
            pltpu.make_async_remote_copy(
                src_ref=ref.at[b, :, thin], dst_ref=kvhalo.at[w, t],
                send_sem=hs_sem.at[w, t], recv_sem=hr_sem.at[w, t],
                device_id=target, device_id_type=MESH,
            )
            for w, ref in enumerate((k_ref, v_ref))
        )

    def grad_copies(t):
        target = (dp, lax.rem(ctx + n_ctx - 1, n_ctx), tp)
        return tuple(
            pltpu.make_async_remote_copy(
                src_ref=gsend.at[w, t], dst_ref=grecv.at[w, t],
                send_sem=gs_sem.at[w, t], recv_sem=gr_sem.at[w, t],
                device_id=target, device_id_type=MESH,
            )
            for w in range(2)
        )

    def sink_copy(i):
        return pltpu.make_async_remote_copy(
            src_ref=ssend, dst_ref=srecv.at[i - 1],
            send_sem=ss_sem.at[i - 1], recv_sem=sr_sem.at[i - 1],
            device_id=peer(i), device_id_type=MESH,
        )

    lane = lax.broadcasted_iota(jnp.int32, (1, LANES), 1)
    low_lane = lane < HEAD
    start = ctx * WINDOW
    for b in range(seqs):
        fold = lax.rem(lane, HALF)
        pos_parts = [start + fold, start + HALF + fold, start - WINDOW + lane, start + lane]
        ids = [jnp.zeros((1, LANES), F32) for _ in pos_parts]
        for d in range(docs):
            s = starts_ref[b, d]
            ids = [x + (s <= pos).astype(F32) for x, pos in zip(ids, pos_parts)]
        key_doc = jnp.concatenate(
            [jnp.transpose(jnp.broadcast_to(x, (LANES, LANES))) for x in ids[2:]], axis=0
        )
        krow = lax.broadcasted_iota(jnp.int32, (2 * WINDOW, LANES), 0)
        kpos = krow - WINDOW
        prev_limit = counts_ref[b, lax.rem(ctx + n_ctx - 1, n_ctx)]
        own_limit = counts_ref[b, ctx]
        first = (ctx == 0).astype(jnp.int32)
        limit = jnp.where(krow < WINDOW, prev_limit * (1 - first), own_limit + WINDOW)
        valid = krow < limit
        for h in range(2):
            qpos = jnp.broadcast_to(h * HALF + fold, (2 * WINDOW, LANES))
            ok = (kpos <= qpos) & (qpos - kpos < WINDOW) & valid & (key_doc == ids[h])
            whole = jnp.where(ok, 0.0, masked_score).astype(F32)
            bias[b, h] = whole[h * HALF : h * HALF + SPAN]

    sacc[...] = jnp.zeros_like(sacc)

    pl.semaphore_wait(barrier, group - 1)

    @pl.when(ctx < n_ctx - 1)
    def _():
        for t in range(chunks):
            for copy in halo_copies(t):
                copy.start()

    @pl.when(ctx == 0)
    def _():
        kvhalo[...] = jnp.zeros_like(kvhalo)

    keep0 = low_lane.astype(F32).astype(BF16)
    keep1 = (1.0 - low_lane.astype(F32)).astype(BF16)

    def spread(tile, ci):
        wide = tile.astype(F32)
        turned = pltpu.roll(wide, HEAD, 1)
        return jnp.where(low_lane, wide, turned) if ci == 0 else jnp.where(low_lane, turned, wide)

    def step(t, carry):
        b, cp = t // pairs, lax.rem(t, pairs)
        for copy in local_copies(t):
            copy.wait()

        @pl.when(ctx > 0)
        def _():
            for copy in halo_copies(t):
                copy.wait_recv()

        kpair = jnp.concatenate([kvhalo[0, t], kvown[0, t]], axis=0)
        vpair = jnp.concatenate([kvhalo[1, t], kvown[1, t]], axis=0)
        sums = []
        for ci in range(2):
            kwide = spread(kpair, ci) * scale
            k2 = kwide.astype(BF16)
            v2 = spread(vpair, ci).astype(BF16)
            dk_parts, dv_parts = [], []
            for h in range(2):
                r0 = h * HALF
                kcut, vcut = k2[r0 : r0 + SPAN], v2[r0 : r0 + SPAN]
                turned = kwide if h == 0 else jnp.concatenate([kwide[HALF:], kwide[:HALF]], axis=0)
                kt = jnp.transpose(turned)[:HEAD, :SPAN].astype(BF16)
                band = bias[b, h]
                band = jnp.concatenate([band, band], axis=1)
                wq_all, wg_all, p_all, d_all = [], [], [], []
                for quad in range(2):
                    base = ci * (qw // 2) + quad * 2 * LANES
                    qs = [qbuf[t, r0 : r0 + HALF, base + p * LANES : base + (p + 1) * LANES] for p in range(2)]
                    gs = [gbuf[t, r0 : r0 + HALF, base + p * LANES : base + (p + 1) * LANES] for p in range(2)]
                    wq = jnp.concatenate([x * keep for keep in (keep0, keep1) for x in qs], axis=0)
                    wg = jnp.concatenate([x * keep for keep in (keep0, keep1) for x in gs], axis=0)
                    head0 = (cp * 2 + ci) * (n_sinks // (2 * pairs)) + quad * 4
                    sink = jnp.concatenate(
                        [
                            jnp.where(low_lane, sinks_ref[head0 + e], sinks_ref[head0 + 2 + e])
                            for e in range(2)
                        ],
                        axis=1,
                    )
                    scores = mm_nt(kcut, wq) + band
                    top = jnp.maximum(jnp.max(scores, axis=0, keepdims=True), sink)
                    powers = jnp.exp(scores - top)
                    sink_exp = jnp.exp(sink - top)
                    inv = 1.0 / (jnp.sum(powers, axis=0, keepdims=True) + sink_exp)
                    prob = powers * inv
                    dprob = mm_nt(vcut, wg)
                    delta = jnp.sum(prob * dprob, axis=0, keepdims=True)
                    dscore = (prob * (dprob - delta)).astype(BF16)
                    dqt = mm(kt, dscore)
                    dq2 = jnp.transpose(jnp.concatenate([dqt[:, :LANES], dqt[:, LANES:]], axis=0)).astype(BF16)
                    for p in range(2):
                        spot = pl.ds(pl.multiple_of(cp * qw + base + p * LANES, LANES), LANES)
                        dq_ref[b, r0 : r0 + HALF, spot] = dq2[p * HALF : (p + 1) * HALF]
                    row = ci * 2 + quad
                    sacc[cp, row : row + 1, :] -= sink_exp * inv * delta
                    wq_all.append(wq)
                    wg_all.append(wg)
                    p_all.append(prob.astype(BF16))
                    d_all.append(dscore)
                dv_parts.append(mm(jnp.concatenate(p_all, axis=1), jnp.concatenate(wg_all, axis=0)))
                dk_parts.append(mm(jnp.concatenate(d_all, axis=1), jnp.concatenate(wq_all, axis=0)))
            totals = []
            for lo, hi in (dk_parts, dv_parts):
                x = jnp.concatenate([lo[:HALF], lo[HALF:] + hi[:WINDOW], hi[WINDOW:]], axis=0)
                totals.append(x + pltpu.roll(x, HEAD, 1))
            sums.append(totals)
        for w in range(2):
            x = jnp.where(low_lane, sums[0][w], sums[1][w])
            if w == 0:
                x = x * scale
            gsend[w, t] = x[:WINDOW].astype(BF16)
            gown[w, t] = x[WINDOW:]

        @pl.when(ctx > 0)
        def _():
            for copy in grad_copies(t):
                copy.start()

        return carry

    lax.fori_loop(0, chunks, step, 0)

    lane4 = lax.broadcasted_iota(jnp.int32, (4, LANES), 1)
    row4 = lax.broadcasted_iota(jnp.int32, (4, LANES), 0)
    mine = jnp.zeros((1, LANES), F32)
    for cp in range(pairs):
        part = sacc[cp]
        for e in range(2):
            cut = part[:, e * LANES : (e + 1) * LANES]
            for p in range(2):
                chosen = low_lane if p == 0 else jnp.logical_not(low_lane)
                seg = jnp.sum(jnp.where(chosen, cut, 0.0), axis=1, keepdims=True)
                spot = lane4 == cp * 16 + row4 * 4 + p * 2 + e
                mine = mine + jnp.sum(jnp.where(spot, seg, 0.0), axis=0, keepdims=True)
    ssend[...] = jnp.broadcast_to(mine, ssend.shape)

    def send_sink(i, carry):
        sink_copy(i).start()
        return carry

    lax.fori_loop(1, group, send_sink, 0)

    for t in range(chunks):
        b, cp = t // pairs, t % pairs
        cut = slice(cp * LANES, (cp + 1) * LANES)

        @pl.when(ctx < n_ctx - 1)
        def _():
            for copy in grad_copies(t):
                copy.wait_recv()
            for w, ref in enumerate((dk_ref, dv_ref)):
                ref[b, :, cut] = (gown[w, t] + grecv[w, t].astype(F32)).astype(BF16)

        @pl.when(ctx == n_ctx - 1)
        def _():
            for w, ref in enumerate((dk_ref, dv_ref)):
                ref[b, :, cut] = gown[w, t].astype(BF16)

    @pl.when(ctx < n_ctx - 1)
    def _():
        for t in range(chunks):
            for copy in halo_copies(t):
                copy.wait_send()

    @pl.when(ctx > 0)
    def _():
        for t in range(chunks):
            for copy in grad_copies(t):
                copy.wait_send()

    def take_sink(i, total):
        sink_copy(i).wait()
        return total + srecv[i - 1]

    total = lax.fori_loop(1, group, take_sink, ssend[...])
    sg_ref[...] = total[:1, : sg_ref.shape[1]]


def write_out(*refs):
    sems = refs[-1]
    copies = [pltpu.make_async_copy(refs[i], refs[4 + i], sems.at[i]) for i in range(4)]
    for copy in copies:
        copy.start()
    for copy in copies:
        copy.wait()


def local(n_dp, n_ctx, queries, keys, values, output_gradient, sinks, doc_starts, valid_counts):
    seqs, rows, query_width = queries.shape
    kv_width = keys.shape[2]
    assert rows == WINDOW and kv_width % LANES == 0
    pairs = kv_width // LANES
    assert query_width == kv_width * 8
    chunks = seqs * pairs
    group = n_dp * n_ctx
    hbm = pl.BlockSpec(memory_space=pltpu.HBM)
    vmem = pl.BlockSpec(memory_space=pltpu.VMEM)
    wide = query_width // pairs
    dq, dk, dv, sg = pl.pallas_call(
        functools.partial(kernel, n_dp, n_ctx, seqs, pairs),
        out_shape=(
            jax.ShapeDtypeStruct(queries.shape, BF16),
            jax.ShapeDtypeStruct(keys.shape, BF16),
            jax.ShapeDtypeStruct(values.shape, BF16),
            jax.ShapeDtypeStruct((1, sinks.shape[0]), F32),
        ),
        in_specs=[hbm] * 7,
        out_specs=(vmem, vmem, vmem, vmem),
        scratch_shapes=[
            pltpu.VMEM((chunks, rows, wide), BF16),
            pltpu.VMEM((chunks, rows, wide), BF16),
            pltpu.VMEM((2, chunks, rows, LANES), BF16),
            pltpu.VMEM((2, chunks, rows, LANES), BF16),
            pltpu.SMEM(sinks.shape, F32),
            pltpu.SMEM(doc_starts.shape, jnp.int32),
            pltpu.SMEM(valid_counts.shape, jnp.int32),
            pltpu.VMEM((seqs, 2, SPAN, LANES), F32),
            pltpu.VMEM((2, chunks, rows, LANES), BF16),
            pltpu.VMEM((2, chunks, rows, LANES), BF16),
            pltpu.VMEM((2, chunks, rows, LANES), F32),
            pltpu.VMEM((pairs, 4, 2 * LANES), F32),
            pltpu.VMEM((8, LANES), F32),
            pltpu.VMEM((group - 1, 8, LANES), F32),
            pltpu.SemaphoreType.DMA((4, chunks)),
            pltpu.SemaphoreType.DMA((3,)),
            pltpu.SemaphoreType.DMA((2, chunks)),
            pltpu.SemaphoreType.DMA((2, chunks)),
            pltpu.SemaphoreType.DMA((2, chunks)),
            pltpu.SemaphoreType.DMA((2, chunks)),
            pltpu.SemaphoreType.DMA((group - 1,)),
            pltpu.SemaphoreType.DMA((group - 1,)),
        ],
        compiler_params=pltpu.CompilerParams(
            collective_id=0, has_side_effects=True, vmem_limit_bytes=67_043_328
        ),
    )(queries, keys, values, output_gradient, sinks, doc_starts, valid_counts)
    results = (dq, dk, dv, sg)
    dq, dk, dv, sg = pl.pallas_call(
        write_out,
        out_shape=tuple(jax.ShapeDtypeStruct(x.shape, x.dtype) for x in results),
        in_specs=[vmem] * 4,
        out_specs=(hbm,) * 4,
        scratch_shapes=[pltpu.SemaphoreType.DMA((4,))],
    )(*results)
    return dq, dk, dv, sg.reshape(sinks.shape)


def solution(mesh):
    placed = (
        P("dp", "ctx", "tp"),
        P("dp", "ctx", "tp"),
        P("dp", "ctx", "tp"),
        P("dp", "ctx", "tp"),
        P("tp"),
        P("dp", None),
        P("dp", None),
    )
    return jax.shard_map(
        functools.partial(local, mesh.shape["dp"], mesh.shape["ctx"]),
        mesh=mesh,
        in_specs=placed,
        out_specs=(P("dp", "ctx", "tp"), P("dp", "ctx", "tp"), P("dp", "ctx", "tp"), P("tp")),
        check_vma=False,
    )
```
